256 devices in a mesh: grp: 32 (over y_hi, z, core), col: 8 (over x, y_lo).
Axes of the slice: x: 4, y: 4 (y_hi: 2, y_lo: 2; y = y_hi * 2 + y_lo), z: 8, core: 2. Of those that a mesh axis runs over, the one named last changes fastest.
Arguments:
- grad: float32 [4096, 16384], P('col', 'grp'), may hold values from -1.8 to 1.8
- exp_avg: float32 [4096, 16384], P('col', 'grp'), may hold values from -1.8 to 1.8
- exp_avg_sq: float32 [4096, 16384], P('col', 'grp'), may hold values from 0.01 to 0.36
- left_basis: bfloat16 [4096, 4096], P('grp', 'col'), may hold values from -1 to 1
- right_basis: bfloat16 [16384, 512], P('grp', 'col'), may hold values from -1 to 1
- gram_left: float32 [4096, 4096], P('grp', 'col'), may hold values from -6 to 6
- gram_right: float32 [16384, 512], P('grp', 'col'), may hold values from -6 to 6
Outputs:
- update: float32 [4096, 16384], P('col', 'grp')
- first_moment: float32 [4096, 16384], P('col', 'grp')
- second_moment: float32 [4096, 16384], P('col', 'grp')
- left_stat: float32 [4096, 4096], P('grp', 'col')
- right_stat: float32 [16384, 512], P('grp', 'col')
The draws below stay inside these ranges and needn't reach their ends.
All inputs are finite; a program needn't handle non-finite values.
Results may differ from the reference program's by a relative error of at most 0.0041.
Values may be sent and summed in bfloat16 or wider, within the bound.
A program may use at most 128 MiB of HBM per device.

```python
import math
import jax
import jax.numpy as jnp
from jax import lax

M = 4096
N = 16384
RB = 512


def draw_left_basis(key, part):
    noise = jax.random.normal(jax.random.fold_in(key, 11), (M, M), jnp.float32)
    basis, upper = jnp.linalg.qr(noise)
    return basis.astype(jnp.bfloat16)


def draw_right_basis(key, part):
    noise = jax.random.normal(jax.random.fold_in(key, 23), (N // RB, RB, RB), jnp.float32)
    basis, upper = jnp.linalg.qr(noise)
    return basis.reshape(N, RB).astype(jnp.bfloat16)


def raised(entries, key, source, target, blocks, factor):
    owner, partner = [(jnp.arange(entries.shape[axis_at]) // (entries.shape[axis_at] // blocks)).reshape([-1 if axis == axis_at else 1 for axis in range(entries.ndim)]) for axis_at in (source, target)]
    chosen = jax.random.permutation(key, blocks)[partner]
    strong = (owner == chosen) | (owner == (partner + blocks // 2) % blocks)
    return jnp.where(strong, factor * entries, entries)


def block_scale(rng, shape, shards, least, largest):
    def one(dim, blocks):
        heights = jax.random.uniform(jax.random.fold_in(jax.random.fold_in(rng, 6), dim), (blocks,), jnp.float32, least / len(shards), largest / len(shards))
        return jnp.repeat(jnp.exp(heights), shape[dim] // blocks).reshape((-1,) + (1,) * (len(shape) - dim - 1))

    factor_of = one(*shards[0])
    for cut in shards[1:]:
        factor_of = factor_of * one(*cut)
    return factor_of


def gaussian(stream_key, extent, width, most, cuts=(), kind=jnp.bfloat16):
    entries = jax.random.normal(stream_key, extent, jnp.float32) * width
    if len(cuts) > 0:
        entries = block_scale(stream_key, extent, cuts, -0.22, 0.18) * entries
    return jnp.clip(entries, min=-most, max=most).astype(kind)


def gaussian_with(rng, extent, scale, bound, cuts, heavy, kind=jnp.bfloat16):
    drawn = scale * jax.random.normal(rng, extent, jnp.float32)
    if cuts:
        drawn = drawn * block_scale(rng, extent, cuts, -0.22, 0.18)
    return jnp.clip(raised(drawn, jax.random.fold_in(rng, 3), *heavy), -bound, bound).astype(kind)


def setup_inputs(seed: int = 0) -> dict:
    streams_of = jax.random.split(jax.random.key(seed), 8)
    grad = gaussian_with(streams_of[0], (M, N), 0.3, 1.8, ((0, 8), (1, 32)), (1, 0, 32, 2.75), jnp.float32)
    exp_avg = gaussian(streams_of[1], (M, N), 0.3, 1.8, ((0, 8), (1, 32)), jnp.float32)
    exp_avg_sq = jnp.clip(jnp.exp(math.log(0.36) - 3.583519 * jax.random.uniform(streams_of[2], (M, N), jnp.float32) ** block_scale(streams_of[2], (M, N), ((0, 8), (1, 32)), -0.2, 0.2)), 0.01, 0.36)
    left_basis = draw_left_basis(jax.random.fold_in(streams_of[7], 71), 0)
    right_basis = draw_right_basis(jax.random.fold_in(streams_of[7], 71), 0)
    gram_left = gaussian(streams_of[5], (M, M), 1.0, 6.0, ((0, 32), (1, 8)), jnp.float32)
    gram_right = gaussian(streams_of[6], (N, RB), 1.0, 6.0, ((0, 32), (1, 8)), jnp.float32)
    return dict(grad=grad, exp_avg=exp_avg, exp_avg_sq=exp_avg_sq, left_basis=left_basis, right_basis=right_basis, gram_left=gram_left, gram_right=gram_right)


decay = 0.95
bias_fix = 1.0 - decay ** 10

def reference(grad, exp_avg, exp_avg_sq, left_basis, right_basis, gram_left, gram_right):
    block_count = N // RB
    rounded = grad.astype(jnp.bfloat16)
    grad_blocks = rounded.reshape(M, block_count, RB).astype(jnp.float32)
    basis_blocks = right_basis.reshape(block_count, RB, RB).astype(jnp.float32)
    turned = jnp.einsum('mbj,bjr->mbr', grad_blocks, basis_blocks, precision=lax.Precision.HIGHEST)
    turned = turned.reshape(M, N).astype(jnp.bfloat16)
    rotated = jnp.dot(left_basis.T.astype(jnp.float32), turned.astype(jnp.float32), preferred_element_type=jnp.float32)
    first_moment = decay * exp_avg + (1.0 - decay) * rotated
    second_moment = decay * exp_avg_sq + (1.0 - decay) * rotated * rotated
    direction = (first_moment / bias_fix / (jnp.sqrt(second_moment / bias_fix) + 1e-08)).astype(jnp.bfloat16)
    back = jnp.dot(left_basis.astype(jnp.float32), direction.astype(jnp.float32), preferred_element_type=jnp.float32).astype(jnp.bfloat16)
    back_blocks = back.reshape(M, block_count, RB).astype(jnp.float32)
    update = jnp.einsum('mbr,bjr->mbj', back_blocks, basis_blocks, precision=lax.Precision.HIGHEST).reshape(M, N)
    left_stat = decay * gram_left + (1.0 - decay) * jnp.dot(rounded.astype(jnp.float32), rounded.T.astype(jnp.float32), preferred_element_type=jnp.float32)
    right_term = jnp.einsum('mbj,mbr->bjr', grad_blocks, grad_blocks, precision=lax.Precision.HIGHEST).reshape(N, RB)
    right_stat = decay * gram_right + (1.0 - decay) * right_term
    return (update, first_moment, second_moment, left_stat, right_stat)
```

```python
import functools

import jax
import jax.numpy as jnp
from jax import lax
from jax.experimental import pallas as pl
from jax.experimental.pallas import tpu as pltpu
from jax.sharding import PartitionSpec as P

decay = 0.95
bias_fix = 1.0 - decay**10
B16 = jnp.bfloat16
F32 = jnp.float32
BY_ROWS = (((1,), (1,)), ((), ()))
PLAIN = (((1,), (0,)), ((), ()))


def dot(a, b, dims=PLAIN):
    return lax.dot_general(a, b, dims, preferred_element_type=F32)


def kernel(
    grad, exp_avg, exp_avg_sq, left, right_t, gram_left, gram_right,
    update, first, second, left_stat, right_stat,
    G, R, L, LT, T, LP, EP, rot, right_acc, dirn,
    ER, ES, AO, YB, D1, D1Y, D2, D2Y, D3, S1, S1Y, S2, S2Y, S3,
    send_sem, g_sem, r_sem, l_sem, e_sem, er_sem, yb_sem, d1_sem, d1y_sem, d2_sem, d2y_sem, d3_sem,
):
    grp = lax.axis_index("grp")
    col = lax.axis_index("col")
    core = grp % 2
    z = (grp // 2) % 8
    yh = grp // 16
    x = col // 2
    yl = col % 2

    def z_at(k, half=None, c=None):
        h = yh if half is None else half
        cc = core if c is None else c
        return h * 16 + ((z + k + 8) % 8) * 2 + cc

    def c_at(k, flip=0):
        return ((x + k + 4) % 4) * 2 + (yl if flip == 0 else 1 - yl)

    oh = 1 - yh
    oc = 1 - core
    XP = {"grp": grp, "col": c_at(1)}
    XM = {"grp": grp, "col": c_at(-1)}
    YN = {"grp": grp, "col": c_at(0, 1)}
    ZP = {"grp": z_at(1), "col": col}
    ZM = {"grp": z_at(-1), "col": col}
    YF = {"grp": z_at(0, oh), "col": col}
    CO = {"grp": z_at(0, None, oc), "col": col}

    sends = []

    def send(src, dst, sem, to):
        cp = pltpu.make_async_remote_copy(
            src_ref=src, dst_ref=dst, send_sem=send_sem.at[len(sends)], recv_sem=sem,
            device_id=to, device_id_type=pl.DeviceIdType.MESH,
        )
        cp.start()
        sends.append(cp)

    def arrived(dst, sem):
        pltpu.make_async_remote_copy(
            src_ref=dst, dst_ref=dst, send_sem=send_sem.at[0], recv_sem=sem,
            device_id=XP, device_id_type=pl.DeviceIdType.MESH,
        ).wait_recv()

    H = G.shape[1] // 2
    W = R.shape[1] // 2

    def g_half(s, h):
        return G.at[s, pl.ds(h * H, H)]

    def r_half(s, h):
        return R.at[s, pl.ds(h * W, W)]

    def send_g(s, h, to):
        send(g_half(s, h), g_half(s, h), g_sem.at[s, h], to)

    def send_r(s, h, to):
        send(r_half(s, h), r_half(s, h), r_sem.at[s, h], to)

    def got_g(s, h):
        arrived(g_half(s, h), g_sem.at[s, h])

    def got_r(s, h):
        arrived(r_half(s, h), r_sem.at[s, h])

    def send_l(g, to):
        send(L.at[g], L.at[g], l_sem.at[g], to)

    def got_l(g):
        arrived(L.at[g], l_sem.at[g])

    G[col] = grad[...].astype(B16)
    R[col] = right_t[...]
    L[grp] = left[...]
    right_acc[...] = jnp.zeros_like(right_acc)
    rot[...] = jnp.zeros_like(rot)
    barrier = pltpu.get_barrier_semaphore()
    for to in (XP, XM, YN, ZP, ZM, YF, CO):
        pl.semaphore_signal(barrier, inc=1, device_id=to, device_id_type=pl.DeviceIdType.MESH)
    pl.semaphore_wait(barrier, 7)

    me = col
    xm, xp, yn = c_at(-1), c_at(1), c_at(0, 1)
    far = c_at(2)
    xm_n, xp_n, far_n = c_at(-1, 1), c_at(1, 1), c_at(2, 1)

    for h in (0, 1):
        for to in (YN, XP, XM):
            send_r(me, h, to)
    for to in (YF, ZP, ZM, CO):
        send_l(grp, to)
    for to in (YN, XP, XM):
        send_g(me, 0, to)

    def l_pass(g, to):
        got_l(g)
        if to is not None:
            send_l(g, to)
        send_l(g, CO)

    for h in (0, 1):
        got_r(xm, h)
        if h == 0:
            send_r(xm, 0, XP)
        got_r(xp, h)
        if h == 1:
            send_r(xp, 1, XM)
        got_r(yn, h)
        send_r(yn, h, XP)
        send_r(yn, h, XM)
    for to in (YN, XP, XM):
        send_g(me, 1, to)
    g = z_at(0, oh)
    got_l(g)
    send_l(g, ZP)
    send_l(g, ZM)
    send_l(g, CO)
    l_pass(z_at(-1), ZP)
    l_pass(z_at(1), ZM)
    l_pass(z_at(-1, oh), ZP)
    l_pass(z_at(1, oh), ZM)

    got_g(xm, 0)
    send_g(xm, 0, XP)
    got_g(yn, 0)
    send_g(yn, 0, XP)
    send_g(yn, 0, XM)
    got_g(xp, 0)
    got_r(far, 0)
    send_r(far, 0, YN)
    got_r(far, 1)
    send_r(far, 1, YN)

    l_pass(z_at(-2), ZP)
    l_pass(z_at(2), ZM)
    l_pass(z_at(-2, oh), ZP)
    l_pass(z_at(2, oh), ZM)

    got_g(xp, 1)
    send_g(xp, 1, XM)
    got_g(yn, 1)
    send_g(yn, 1, XP)
    send_g(yn, 1, XM)
    got_g(xm, 1)

    l_pass(z_at(-3), ZP)
    l_pass(z_at(3), None)
    l_pass(z_at(-3, oh), None)
    l_pass(z_at(3, oh), ZM)

    for s in (xm_n, xp_n, far_n):
        got_r(s, 0)
        got_r(s, 1)

    width = right_stat.shape[1]
    RB = G.shape[2]
    picks = lax.broadcasted_iota(jnp.int32, (128, RB), 0)
    lanes = lax.broadcasted_iota(jnp.int32, (128, RB), 1)
    chosen = jnp.where(
        jnp.logical_and(picks < width, lanes == picks + col * width), 1.0, 0.0
    ).astype(B16)

    def piece(s):
        rows = G[s]
        T[s] = dot(rows, R[...].reshape(RB, RB), BY_ROWS).astype(B16)
        LP[pl.ds(2 * s, 2)] = dot(rows, G[me], BY_ROWS).reshape(2, 2, 128, RB)
        narrow = dot(chosen, rows, BY_ROWS).astype(B16)
        right_acc[...] += dot(narrow, rows)

    def pair_send(s):
        send(
            LP.at[pl.ds(2 * s, 2), oc], EP.at[pl.ds(2 * s, 2)], e_sem.at[s], CO
        )

    def near_piece(i, carry):
        dx = jnp.where(i == 1, 3, jnp.where(i == 2, 1, 0))
        y = jnp.where(i == 3, 1 - yl, yl)
        piece(((x + dx) % 4) * 2 + y)
        return carry

    lax.fori_loop(0, 4, near_piece, 0)
    for s in (me, xm, xp, yn):
        pair_send(s)

    got_g(far, 0)
    send_g(far, 0, YN)
    got_g(far, 1)
    send_g(far, 1, YN)
    l_pass(z_at(4), None)
    l_pass(z_at(4, oh), None)
    for h in (yh, oh):
        for k in range(8):
            got_l(z_at(k, h, oc))

    def turn_left(r, carry):
        block = L[pl.ds(4 * r, 4)].reshape(RB, RB)
        LT[r] = block.T
        return carry

    lax.fori_loop(0, 8, turn_left, 0)

    for s in (xm_n, xp_n):
        got_g(s, 0)
        got_g(s, 1)
    got_g(far_n, 0)
    got_g(far_n, 1)

    def far_piece(i, carry):
        dx = jnp.where(i == 1, 3, jnp.where(i == 2, 1, 2))
        y = jnp.where(i == 0, yl, 1 - yl)
        piece(((x + dx) % 4) * 2 + y)
        return carry

    lax.fori_loop(0, 4, far_piece, 0)
    for s in (far, xm_n, xp_n, far_n):
        pair_send(s)

    def rotate(r, carry):
        rot[...] += dot(LT[r], T[r])
        return carry

    lax.fori_loop(0, 8, rotate, 0)

    def moments(i, carry):
        at = pl.ds(i * 64, 64)
        turned = rot[at, :]
        m1 = decay * exp_avg[at, :] + (1.0 - decay) * turned
        m2 = decay * exp_avg_sq[at, :] + (1.0 - decay) * turned * turned
        first[at, :] = m1
        second[at, :] = m2
        dirn[at, :] = (m1 / bias_fix / (jnp.sqrt(m2 / bias_fix) + 1e-08)).astype(B16)
        return carry

    lax.fori_loop(0, RB // 64, moments, 0)

    def back_of(d):
        return dot(L[pl.ds(4 * d, 4)].reshape(RB, RB), dirn[...])

    def half_of(d, h):
        block = L[pl.ds(4 * d, 4)].reshape(RB, RB)[h * H : (h + 1) * H]
        return dot(block, dirn[...])

    S1Y[...] = back_of(far_n).astype(B16)
    S1[0] = back_of(xp_n).astype(B16)
    S1[1] = back_of(xm_n).astype(B16)
    rows = [pl.ds(0, H), pl.ds(H, H)]
    for h in (0, 1):
        send(S1Y.at[rows[h]], D1Y.at[rows[h]], d1y_sem.at[h], YN)
    send(S1.at[0], D1.at[0], d1_sem.at[0], XP)
    send(S1.at[1], D1.at[1], d1_sem.at[1], XM)

    for s in (me, xm, xp, yn, far, xm_n, xp_n, far_n):
        arrived(EP.at[pl.ds(2 * s, 2)], e_sem.at[s])

    def stat_of(half, k):
        b = half * 8 + (z + k + 8) % 8
        return LP[b, core] + EP[b]

    def stat_step(step):
        for d in (0, 1):
            for k, half in ((0, yh), (1, oh)):
                length = 4 if d == k else 3
                if step > length:
                    continue
                away = length + 1 - step
                total = stat_of(half, away if d == 0 else -away)
                if step > 1:
                    arrived(ER.at[d, k, step - 2], er_sem.at[d, k, step - 2])
                    total = total + ER[d, k, step - 2].astype(F32)
                ES[d, k, step - 1] = total.astype(B16)
                send(
                    ES.at[d, k, step - 1], ER.at[d, k, step - 1],
                    er_sem.at[d, k, step - 1], ZP if d == 0 else ZM,
                )

    def stat_total(k):
        total = stat_of(yh if k == 0 else oh, 0)
        for d in (0, 1):
            last = 3 if d == k else 2
            arrived(ER.at[d, k, last], er_sem.at[d, k, last])
            total = total + ER[d, k, last].astype(F32)
        return total

    stat_step(1)
    S3[0, rows[1]] = half_of(xp, 1).astype(B16)
    S3[1, rows[0]] = half_of(xm, 0).astype(B16)

    arrived(D1Y.at[rows[0]], d1y_sem.at[0])
    S2[0] = (half_of(far, 0) + D1Y[rows[0]].astype(F32)).astype(B16)
    send(S2.at[0], D2.at[0], d2_sem.at[0], XP)
    send(S3.at[0, rows[1]], D3.at[0, rows[1]], d3_sem.at[0, 1], XP)
    send(S3.at[1, rows[0]], D3.at[1, rows[0]], d3_sem.at[1, 0], XM)

    stat_step(2)
    arrived(D1Y.at[rows[1]], d1y_sem.at[1])
    S2[1] = (half_of(far, 1) + D1Y[rows[1]].astype(F32)).astype(B16)
    send(S2.at[1], D2.at[1], d2_sem.at[1], XM)
    arrived(D1.at[0], d1_sem.at[0])
    arrived(D1.at[1], d1_sem.at[1])
    S2Y[...] = (back_of(yn) + D1[0].astype(F32) + D1[1].astype(F32)).astype(B16)
    send(S2Y, D2Y, d2y_sem.at[0], YN)

    stat_step(3)
    right_stat[...] = decay * gram_right[...] + (1.0 - decay) * right_acc[...].T[:, :width]
    arrived(D2.at[0], d2_sem.at[0])
    S3[0, rows[0]] = (half_of(xp, 0) + D2[0].astype(F32)).astype(B16)
    send(S3.at[0, rows[0]], D3.at[0, rows[0]], d3_sem.at[0, 0], XP)
    arrived(D2.at[1], d2_sem.at[1])
    S3[1, rows[1]] = (half_of(xm, 1) + D2[1].astype(F32)).astype(B16)
    send(S3.at[1, rows[1]], D3.at[1, rows[1]], d3_sem.at[1, 1], XM)
    stat_step(4)
    AO[...] = stat_total(1).astype(B16)
    send(AO, YB, yb_sem.at[0], YF)
    left_stat[...] = decay * gram_left[...] + (1.0 - decay) * stat_total(0)

    rot[...] = back_of(me)
    arrived(D2Y, d2y_sem.at[0])
    for h in (0, 1):
        for d in (0, 1):
            arrived(D3.at[d, rows[h]], d3_sem.at[d, h])
    back = rot[...] + D2Y[...].astype(F32) + (D3[0].astype(F32) + D3[1].astype(F32))
    update[...] = dot(back.astype(B16), R[...].reshape(RB, RB))
    arrived(YB, yb_sem.at[0])
    left_stat[...] += (1.0 - decay) * YB[...].astype(F32)
    for cp in sends:
        cp.wait_send()


def local(grad, exp_avg, exp_avg_sq, left_basis, right_basis, gram_left, gram_right):
    rows, RB = grad.shape
    assert rows == RB
    H = RB // 2
    width = right_basis.shape[1]
    vm = pltpu.VMEM
    dma = pltpu.SemaphoreType.DMA
    scratch = [
        vm((8, RB, RB), B16),
        vm((8, width, RB), B16),
        vm((32, 128, RB), B16),
        vm((8, RB, RB), B16),
        vm((8, RB, RB), B16),
        vm((16, 2, 128, RB), F32),
        vm((16, 128, RB), F32),
        vm((RB, RB), F32),
        vm((128, RB), F32),
        vm((RB, RB), B16),
        vm((2, 2, 4, 128, RB), B16),
        vm((2, 2, 4, 128, RB), B16),
        vm((128, RB), B16),
        vm((128, RB), B16),
        vm((2, RB, RB), B16),
        vm((RB, RB), B16),
        vm((2, H, RB), B16),
        vm((RB, RB), B16),
        vm((2, RB, RB), B16),
        vm((2, RB, RB), B16),
        vm((RB, RB), B16),
        vm((2, H, RB), B16),
        vm((RB, RB), B16),
        vm((2, RB, RB), B16),
        dma((128,)), dma((8, 2)), dma((8, 2)), dma((32,)), dma((8,)), dma((2, 2, 4)),
        dma((1,)), dma((2,)), dma((2,)), dma((2,)), dma((1,)), dma((2, 2)),
    ]
    whole = pl.BlockSpec(memory_space=pltpu.VMEM)
    like = lambda a: jax.ShapeDtypeStruct(a.shape, F32)
    return pl.pallas_call(
        kernel,
        out_shape=(like(grad), like(grad), like(grad), like(gram_left), like(gram_right)),
        in_specs=[whole] * 7,
        out_specs=(whole,) * 5,
        scratch_shapes=scratch,
        compiler_params=pltpu.CompilerParams(
            collective_id=0, has_side_effects=True, vmem_limit_bytes=64 * 1024 * 1024 - 65536
        ),
    )(grad, exp_avg, exp_avg_sq, left_basis, right_basis.T, gram_left, gram_right)


def solution(mesh):
    a, b = P("col", "grp"), P("grp", "col")
    return jax.shard_map(
        local, mesh=mesh, in_specs=(a, a, a, b, b, b, b), out_specs=(a, a, a, b, b), check_vma=False
    )
```

```python
import functools

import jax
import jax.numpy as jnp
from jax import lax
from jax.experimental import pallas as pl
from jax.experimental.pallas import tpu as pltpu
from jax.sharding import PartitionSpec as P

decay = 0.95
bias_fix = 1.0 - decay**10
B16 = jnp.bfloat16
F32 = jnp.float32
BY_ROWS = (((1,), (1,)), ((), ()))
BY_COLS = (((0,), (0,)), ((), ()))
PLAIN = (((1,), (0,)), ((), ()))


def dot(a, b, dims=PLAIN):
    return lax.dot_general(a, b, dims, preferred_element_type=F32)


def kernel(
    grad, exp_avg, exp_avg_sq, left, right_t, gram_left, gram_right,
    update, first, second, left_stat, right_stat,
    grad_v, avg_v, sq_v, gl_v, gr_v, G, R, L, T, LP, EP, rot, right_acc, dirn,
    ER, ES, AO, YB, D1, D1Y, X1, D2, D2Y, D3, S1, S1Y, S2, S2Y, S3,
    in_sem, send_sem, g_sem, r_sem, l_sem, e_sem, er_sem, yb_sem, d1_sem, d1y_sem, x1_sem, d2_sem, d2y_sem, d3_sem,
):
    grp = lax.axis_index("grp")
    col = lax.axis_index("col")
    core = grp % 2
    z = (grp // 2) % 8
    yh = grp // 16
    x = col // 2
    yl = col % 2

    def z_at(k, half=None, c=None):
        h = yh if half is None else half
        cc = core if c is None else c
        return h * 16 + ((z + k + 8) % 8) * 2 + cc

    def c_at(k, flip=0):
        return ((x + k + 4) % 4) * 2 + (yl if flip == 0 else 1 - yl)

    oh = 1 - yh
    oc = 1 - core
    XP = {"grp": grp, "col": c_at(1)}
    XM = {"grp": grp, "col": c_at(-1)}
    YN = {"grp": grp, "col": c_at(0, 1)}
    ZP = {"grp": z_at(1), "col": col}
    ZM = {"grp": z_at(-1), "col": col}
    YF = {"grp": z_at(0, oh), "col": col}
    CO = {"grp": z_at(0, None, oc), "col": col}

    sends = []

    def send(src, dst, sem, to):
        cp = pltpu.make_async_remote_copy(
            src_ref=src, dst_ref=dst, send_sem=send_sem.at[len(sends)], recv_sem=sem,
            device_id=to, device_id_type=pl.DeviceIdType.MESH,
        )
        cp.start()
        sends.append(cp)

    def arrived(dst, sem):
        pltpu.make_async_remote_copy(
            src_ref=dst, dst_ref=dst, send_sem=send_sem.at[0], recv_sem=sem,
            device_id=XP, device_id_type=pl.DeviceIdType.MESH,
        ).wait_recv()

    RB = G.shape[2]
    H = RB // 2
    Q = RB // 4
    W = R.shape[1] // 2

    def g_part(s, q):
        return G.at[s, pl.ds(q * Q, Q)]

    def r_half(s, h):
        return R.at[s, pl.ds(h * W, W)]

    def send_g(s, q, to):
        send(g_part(s, q), g_part(s, q), g_sem.at[s, q], to)

    def send_r(s, h, to):
        send(r_half(s, h), r_half(s, h), r_sem.at[s, h], to)

    def got_g(s, *qs):
        for q in qs:
            arrived(g_part(s, q), g_sem.at[s, q])

    def got_r(s, *hs):
        for h in hs:
            arrived(r_half(s, h), r_sem.at[s, h])

    def send_l(g, to):
        send(L.at[g], L.at[g], l_sem.at[g], to)

    def got_l(g):
        arrived(L.at[g], l_sem.at[g])

    barrier = pltpu.get_barrier_semaphore()
    for to in (XP, XM, YN, ZP, ZM, YF, CO):
        pl.semaphore_signal(barrier, inc=1, device_id=to, device_id_type=pl.DeviceIdType.MESH)
    fetches = []
    for k, (src, dst) in enumerate((
        (grad, grad_v), (right_t, R.at[col]), (left, L.at[grp]),
        (exp_avg, avg_v), (exp_avg_sq, sq_v), (gram_left, gl_v), (gram_right, gr_v),
    )):
        cp = pltpu.make_async_copy(src, dst, in_sem.at[k])
        cp.start()
        fetches.append(cp)
    right_acc[...] = jnp.zeros_like(right_acc)
    rot[...] = jnp.zeros_like(rot)
    fetches[0].wait()
    G[col] = grad_v[...].astype(B16)
    fetches[1].wait()
    fetches[2].wait()
    pl.semaphore_wait(barrier, 7)

    me = col
    xm, xp, yn = c_at(-1), c_at(1), c_at(0, 1)
    far = c_at(2)
    xm_n, xp_n, far_n = c_at(-1, 1), c_at(1, 1), c_at(2, 1)

    for h in (0, 1):
        for to in (YN, XP, XM):
            send_r(me, h, to)
    for to in (ZP, ZM, YF, CO):
        send_l(grp, to)
    send_g(me, 0, XP)
    send_g(me, 3, XM)
    send_g(me, 0, YN)

    def l_pass(g, to):
        got_l(g)
        if to is not None:
            send_l(g, to)
        send_l(g, CO)

    width = right_acc.shape[0]
    picks = lax.broadcasted_iota(jnp.int32, (width, RB), 0)
    lanes = lax.broadcasted_iota(jnp.int32, (width, RB), 1)
    chosen = jnp.where(lanes == picks + col * width, 1.0, 0.0).astype(B16)

    def right_of(s):
        rows = G[s]
        narrow = dot(chosen, rows, BY_ROWS).astype(B16)
        right_acc[...] += dot(narrow, rows)

    def rotate(s):
        rot[...] += dot(L[pl.ds(4 * s, 4)].reshape(RB, RB), T[s], BY_COLS)

    def pair_send(s):
        send(LP.at[pl.ds(2 * s, 2), oc], EP.at[pl.ds(2 * s, 2)], e_sem.at[s], CO)

    order = ((0, 0), (0, 1), (3, 0), (1, 0), (2, 0), (3, 1), (1, 1), (2, 1))

    def over(lo, hi, f):
        def body(i, carry):
            dx = sum(jnp.where(i == n, order[n][0], 0) for n in range(lo, hi))
            flip = sum(jnp.where(i == n, order[n][1], 0) for n in range(lo, hi))
            f(((x + dx) % 4) * 2 + (yl + flip) % 2)
            return carry

        lax.fori_loop(lo, hi, body, 0)

    def rows_of(q):
        return pl.ds(pl.multiple_of(q * Q, Q), Q)

    def half_rows(h):
        return pl.ds(h * H, H)

    def turn_h(s, h):
        T[s, half_rows(h)] = dot(G[s, half_rows(h)], R[...].reshape(RB, RB), BY_ROWS).astype(B16)

    def left_h(s, h):
        LP[2 * s + h] = dot(G[s, half_rows(h)], G[me], BY_ROWS).reshape(2, 128, RB)

    def turn_q(s, q):
        T[s, rows_of(q)] = dot(G[s, rows_of(q)], R[...].reshape(RB, RB), BY_ROWS).astype(B16)

    def left_q(s, q):
        LP[2 * s + q // 2, q % 2] = dot(G[s, rows_of(q)], G[me], BY_ROWS)

    def rotate_q(s, q):
        rot[...] += dot(L[4 * s + q], T[s, rows_of(q)], BY_COLS)

    left_h(me, 0)
    got_r(xm, 0, 1)
    send_r(xm, 0, XP)
    got_r(xp, 0, 1)
    send_r(xp, 1, XM)
    for s in (xm, xp):
        for h in (0, 1):
            send_r(s, h, YN)
    send_g(me, 1, XP)
    send_g(me, 2, XM)
    send_g(me, 1, YN)
    l_pass(z_at(-1), ZP)
    l_pass(z_at(1), ZM)
    g = z_at(0, oh)
    got_l(g)
    send_l(g, ZP)
    send_l(g, ZM)
    send_l(g, CO)
    send_g(me, 2, XP)
    send_g(me, 1, XM)
    got_g(xm, 0)
    send_g(xm, 0, XP)
    got_g(xp, 3)
    send_g(xp, 3, XM)
    left_h(me, 1)
    got_r(far, 0, 1)
    send_r(far, 0, YN)
    send_r(far, 1, YN)
    send_g(me, 2, YN)
    send_g(me, 3, YN)
    pair_send(me)
    l_pass(z_at(-2), ZP)
    l_pass(z_at(2), ZM)
    got_g(xm, 1)
    send_g(xm, 1, XP)
    got_g(xp, 2)
    send_g(xp, 2, XM)
    send_g(me, 3, XP)
    send_g(me, 0, XM)
    for q in (0, 1):
        got_g(yn, q)
        send_g(yn, q, XP)
        send_g(yn, q, XM)
    left_h(yn, 0)
    l_pass(z_at(-1, oh), ZP)
    l_pass(z_at(1, oh), ZM)
    left_h(xm, 0)
    left_h(xp, 1)
    l_pass(z_at(-3), ZP)
    l_pass(z_at(3), None)
    got_r(yn, 0, 1)
    for s in (xm_n, xp_n, far_n):
        got_r(s, 0, 1)
    turn_h(me, 0)
    turn_h(me, 1)
    got_g(yn, 2)
    send_g(yn, 2, XP)
    send_g(yn, 2, XM)
    got_g(far, 0, 3)
    send_g(far, 0, YN)
    send_g(far, 3, YN)
    l_pass(z_at(-2, oh), ZP)
    l_pass(z_at(2, oh), ZM)
    turn_h(yn, 0)
    turn_h(xm, 0)
    turn_h(xp, 1)
    got_g(yn, 3)
    send_g(yn, 3, XP)
    send_g(yn, 3, XM)
    got_g(far, 1, 2)
    send_g(far, 1, YN)
    send_g(far, 2, YN)
    l_pass(z_at(4), None)
    turn_h(yn, 1)
    left_h(yn, 1)
    pair_send(yn)
    for h in (0, 1):
        turn_h(far, h)
        left_h(far, h)
    pair_send(far)
    got_g(xm, 2, 3)
    got_g(xp, 0, 1)
    turn_h(xm, 1)
    left_h(xm, 1)
    l_pass(z_at(-3, oh), None)
    l_pass(z_at(3, oh), ZM)
    turn_h(xp, 0)
    left_h(xp, 0)
    pair_send(xm)
    pair_send(xp)

    far_order = (0, 3, 1, 2)

    def late(n, f):
        def body(i, carry):
            dx = jnp.where(i == 5, 3, jnp.where(i == 6, 1, 2))
            q = jnp.where(i == 7, far_order[n], n)
            f(((x + dx) % 4) * 2 + 1 - yl, q)
            return carry

        lax.fori_loop(5, 8, body, 0)

    def late_got(n):
        got_g(xm_n, n)
        got_g(xp_n, n)
        got_g(far_n, far_order[n])

    for n in (0, 1):
        late_got(n)
        late(n, turn_q)
        late(n, left_q)
    l_pass(z_at(4, oh), None)
    for h in (yh, oh):
        for k in range(8):
            got_l(z_at(k, h, oc))
    over(0, 5, rotate)
    late(0, rotate_q)
    late(1, rotate_q)
    for n in (2, 3):
        late_got(n)
        late(n, turn_q)
        late(n, rotate_q)
        if n == 2:
            late(n, left_q)
    fetches[3].wait()
    fetches[4].wait()

    def moments(i, carry):
        at = pl.ds(i * 64, 64)
        turned = rot[at, :]
        m1 = decay * avg_v[at, :] + (1.0 - decay) * turned
        m2 = decay * sq_v[at, :] + (1.0 - decay) * turned * turned
        first[at, :] = m1
        second[at, :] = m2
        dirn[at, :] = (m1 / bias_fix / (jnp.sqrt(m2 / bias_fix) + 1e-08)).astype(B16)
        return carry

    lax.fori_loop(0, RB // 64, moments, 0)

    E = RB // 8

    def part(d, q, count=1):
        return dot(L[pl.ds(4 * d + q, count)].reshape(count * Q, RB), dirn[...])

    def at_rows(lo, n):
        return pl.ds(lo, n)

    lower, upper, rest, first_e = at_rows(0, H), at_rows(H, H), at_rows(E, H - E), at_rows(0, E)
    quarter = [at_rows(q * Q, Q) for q in range(4)]
    S1[0, lower] = part(xp_n, 0, 2).astype(B16)
    S1[1, lower] = part(xm_n, 0, 2).astype(B16)
    send(S1.at[0, rest], D1.at[0, rest], d1_sem.at[0, 0], XP)
    S1Y[lower] = part(far_n, 0, 2).astype(B16)
    send(S1.at[1, rest], D1.at[1, rest], d1_sem.at[1, 0], XM)
    S1[0, upper] = part(xp_n, 2, 2).astype(B16)
    send(S1Y.at[quarter[0]], D1Y.at[quarter[0]], d1y_sem.at[0], YN)
    S1[1, upper] = part(xm_n, 2, 2).astype(B16)
    send(S1.at[0, upper], D1.at[0, upper], d1_sem.at[0, 1], XP)
    S1Y[upper] = part(far_n, 2, 2).astype(B16)
    send(S1.at[1, upper], D1.at[1, upper], d1_sem.at[1, 1], XM)
    late(3, left_q)
    for q in (2, 1, 3):
        send(S1Y.at[quarter[q]], D1Y.at[quarter[q]], d1y_sem.at[q], YN)
    for d in (0, 1):
        send(S1.at[d, first_e], X1.at[d], x1_sem.at[d], YN)
    for s in (xm_n, xp_n, far_n):
        pair_send(s)
    fetches[5].wait()
    fetches[6].wait()

    def stat_of(half, k):
        b = half * 8 + (z + k + 8) % 8
        return LP[b, core] + EP[b]

    def stat_send(d, k, step):
        length = 4 if d == k else 3
        away = length + 1 - step
        total = stat_of(yh if k == 0 else oh, away if d == 0 else -away)
        if step > 1:
            arrived(ER.at[d, k, step - 2], er_sem.at[d, k, step - 2])
            total = total + ER[d, k, step - 2].astype(F32)
        ES[d, k, step - 1] = total.astype(B16)
        send(
            ES.at[d, k, step - 1], ER.at[d, k, step - 1], er_sem.at[d, k, step - 1],
            ZP if d == 0 else ZM,
        )

    def stat_total(k):
        total = stat_of(yh if k == 0 else oh, 0)
        for d in (0, 1):
            last = 3 if d == k else 2
            arrived(ER.at[d, k, last], er_sem.at[d, k, last])
            total = total + ER[d, k, last].astype(F32)
        return total

    S3[0, upper] = part(xp, 2, 2).astype(B16)
    S3[1, lower] = part(xm, 0, 2).astype(B16)
    for s in (me, xm, xp, yn, far, xm_n, xp_n, far_n):
        arrived(EP.at[pl.ds(2 * s, 2)], e_sem.at[s])
    for k in (1, 0):
        stat_send(0, k, 1)
        stat_send(1, k, 1)

    def second_hop(d, q):
        arrived(D1Y.at[quarter[q]], d1y_sem.at[q])
        own = quarter[q - 2 * d]
        S2[d, own] = (part(far, q) + D1Y[quarter[q]].astype(F32)).astype(B16)
        send(S2.at[d, own], D2.at[d, own], d2_sem.at[d, q - 2 * d], XP if d == 0 else XM)

    over(0, 4, right_of)
    second_hop(0, 0)
    second_hop(1, 2)
    stat_send(0, 1, 2)
    stat_send(1, 1, 2)
    second_hop(0, 1)
    second_hop(1, 3)
    send(S3.at[0, upper], D3.at[0, upper], d3_sem.at[0, 2], XP)
    send(S3.at[1, rest], D3.at[1, rest], d3_sem.at[1, 0], XM)
    stat_send(0, 0, 2)
    stat_send(1, 0, 2)
    for d in (0, 1):
        arrived(D1.at[d, upper], d1_sem.at[d, 1])
        arrived(D1.at[d, rest], d1_sem.at[d, 0])
    S2Y[upper] = (
        part(yn, 2, 2) + D1[0, upper].astype(F32) + D1[1, upper].astype(F32)
    ).astype(B16)
    own = part(yn, 0, 2)
    S2Y[first_e] = own[:E].astype(B16)
    S2Y[rest] = (own[E:] + D1[0, rest].astype(F32) + D1[1, rest].astype(F32)).astype(B16)
    send(S2Y.at[upper], D2Y.at[upper], d2y_sem.at[1], YN)
    send(S2Y.at[lower], D2Y.at[lower], d2y_sem.at[0], YN)
    stat_send(0, 1, 3)
    stat_send(1, 1, 3)
    for d in (0, 1):
        arrived(X1.at[d], x1_sem.at[d])
    S3[1, first_e] = (dot(L[4 * xm, first_e], dirn[...]) + X1[1].astype(F32)).astype(B16)
    send(S3.at[1, first_e], D3.at[1, first_e], d3_sem.at[1, 1], XM)
    arrived(D2.at[0, quarter[0]], d2_sem.at[0, 0])
    own = part(xp, 0) + D2[0, quarter[0]].astype(F32)
    S3[0, first_e] = (own[:E] + X1[0].astype(F32)).astype(B16)
    S3[0, at_rows(E, Q - E)] = own[E:].astype(B16)

    def third_hop(d, q):
        mine = quarter[q - 2 * d]
        arrived(D2.at[d, mine], d2_sem.at[d, q - 2 * d])
        S3[d, quarter[q]] = (
            part(xp if d == 0 else xm, q) + D2[d, mine].astype(F32)
        ).astype(B16)

    def third_send(d, q):
        send(
            S3.at[d, quarter[q]], D3.at[d, quarter[q]], d3_sem.at[d, q],
            XP if d == 0 else XM,
        )

    third_hop(1, 2)
    third_send(0, 0)
    third_send(1, 2)
    stat_send(0, 0, 3)
    third_hop(0, 1)
    third_send(0, 1)
    third_hop(1, 3)
    third_send(1, 3)
    stat_send(1, 1, 4)
    stat_send(1, 0, 3)
    over(4, 8, right_of)
    right_stat[...] = decay * gr_v[...] + (1.0 - decay) * right_acc[...]
    stat_send(0, 0, 4)
    rot[...] = part(me, 0, 4)
    AO[...] = stat_total(1).astype(B16)
    send(AO, YB, yb_sem.at[0], YF)
    left_stat[...] = decay * gl_v[...] + (1.0 - decay) * stat_total(0)
    arrived(D2Y.at[upper], d2y_sem.at[1])
    arrived(D2Y.at[lower], d2y_sem.at[0])
    arrived(D3.at[0, upper], d3_sem.at[0, 2])
    arrived(D3.at[1, rest], d3_sem.at[1, 0])
    arrived(D3.at[1, first_e], d3_sem.at[1, 1])
    rot[upper] += D2Y[upper].astype(F32) + D3[0, upper].astype(F32)
    rot[lower] += D2Y[lower].astype(F32) + D3[1, lower].astype(F32)
    for q in (0, 1):
        arrived(D3.at[0, quarter[q]], d3_sem.at[0, q])
        arrived(D3.at[1, quarter[q + 2]], d3_sem.at[1, q + 2])
    basis = R[...].reshape(RB, RB)
    update[lower] = dot((rot[lower] + D3[0, lower].astype(F32)).astype(B16), basis)
    update[upper] = dot((rot[upper] + D3[1, upper].astype(F32)).astype(B16), basis)
    arrived(YB, yb_sem.at[0])
    left_stat[...] += (1.0 - decay) * YB[...].astype(F32)
    for cp in sends:
        cp.wait_send()


def put_out(*refs):
    held, out, sem = refs[:5], refs[5:10], refs[10]
    copies = [pltpu.make_async_copy(a, b, sem.at[k]) for k, (a, b) in enumerate(zip(held, out))]
    for cp in copies:
        cp.start()
    for cp in copies:
        cp.wait()


def local(grad, exp_avg, exp_avg_sq, left_basis, right_basis, gram_left, gram_right):
    rows, RB = grad.shape
    assert rows == RB
    H = RB // 2
    width = right_basis.shape[1]
    vm = pltpu.VMEM
    dma = pltpu.SemaphoreType.DMA
    scratch = [
        vm((RB, RB), F32), vm((RB, RB), F32), vm((RB, RB), F32), vm((128, RB), F32), vm((width, RB), F32),
        vm((8, RB, RB), B16),
        vm((8, width, RB), B16),
        vm((32, 128, RB), B16),
        vm((8, RB, RB), B16),
        vm((16, 2, 128, RB), F32),
        vm((16, 128, RB), F32),
        vm((RB, RB), F32),
        vm((width, RB), F32),
        vm((RB, RB), B16),
        vm((2, 2, 4, 128, RB), B16),
        vm((2, 2, 4, 128, RB), B16),
        vm((128, RB), B16),
        vm((128, RB), B16),
        vm((2, RB, RB), B16),
        vm((RB, RB), B16),
        vm((2, RB // 8, RB), B16),
        vm((2, H, RB), B16),
        vm((RB, RB), B16),
        vm((2, RB, RB), B16),
        vm((2, RB, RB), B16),
        vm((RB, RB), B16),
        vm((2, H, RB), B16),
        vm((RB, RB), B16),
        vm((2, RB, RB), B16),
        dma((7,)), dma((160,)), dma((8, 4)), dma((8, 2)), dma((32,)), dma((8,)), dma((2, 2, 4)),
        dma((1,)), dma((2, 2)), dma((4,)), dma((2,)), dma((2, 2)), dma((2,)), dma((2, 4)),
    ]
    whole = pl.BlockSpec(memory_space=pl.ANY)
    like = lambda a: pltpu.VMEM(a.shape, F32)
    gram_rt = gram_right.T
    update, first, second, left_stat, right_rt = pl.pallas_call(
        kernel,
        out_shape=(like(grad), like(grad), like(grad), like(gram_left), like(gram_rt)),
        in_specs=[whole] * 7,
        out_specs=(pl.BlockSpec(memory_space=pltpu.VMEM),) * 5,
        scratch_shapes=scratch,
        compiler_params=pltpu.CompilerParams(
            collective_id=0, has_side_effects=True, vmem_limit_bytes=58 * 1024 * 1024
        ),
    )(grad, exp_avg, exp_avg_sq, left_basis, right_basis.T, gram_left, gram_rt)
    results = (update, first, second, left_stat, right_rt)
    update, first, second, left_stat, right_rt = pl.pallas_call(
        put_out,
        out_shape=tuple(jax.ShapeDtypeStruct(a.shape, F32) for a in results),
        in_specs=[pl.BlockSpec(memory_space=pltpu.VMEM)] * 5,
        out_specs=(whole,) * 5,
        scratch_shapes=[dma((5,))],
        compiler_params=pltpu.CompilerParams(vmem_limit_bytes=2 * 1024 * 1024),
    )(*results)
    return update, first, second, left_stat, right_rt.T


def solution(mesh):
    a, b = P("col", "grp"), P("grp", "col")
    return jax.shard_map(
        local, mesh=mesh, in_specs=(a, a, a, b, b, b, b), out_specs=(a, a, a, b, b), check_vma=False
    )
```

```python
import functools

import jax
import jax.numpy as jnp
from jax import lax
from jax.experimental import pallas as pl
from jax.experimental.pallas import tpu as pltpu
from jax.sharding import PartitionSpec as P

decay = 0.95
bias_fix = 1.0 - decay**10
B16 = jnp.bfloat16
F32 = jnp.float32
BY_ROWS = (((1,), (1,)), ((), ()))
BY_COLS = (((0,), (0,)), ((), ()))
PLAIN = (((1,), (0,)), ((), ()))


def dot(a, b, dims=PLAIN):
    return lax.dot_general(a, b, dims, preferred_element_type=F32)


def kernel(
    grad, exp_avg, exp_avg_sq, left, right_t, gram_left, gram_right,
    update, first, second, left_stat, right_stat,
    grad_v, avg_v, sq_v, gl_v, gr_v, G, R, L, T, LP, EP, rot, right_acc, dirn,
    ER, ES, AO, YB, D1, D1Y, X1, D2, D2Y, D3, S1, S1Y, S2, S2Y, S3,
    in_sem, send_sem, g_sem, r_sem, l_sem, e_sem, er_sem, yb_sem, d1_sem, d1y_sem, x1_sem, d2_sem, d2y_sem, d3_sem,
):
    grp = lax.axis_index("grp")
    col = lax.axis_index("col")
    core = grp % 2
    z = (grp // 2) % 8
    yh = grp // 16
    x = col // 2
    yl = col % 2

    def z_at(k, half=None, c=None):
        h = yh if half is None else half
        cc = core if c is None else c
        return h * 16 + ((z + k + 8) % 8) * 2 + cc

    def c_at(k, flip=0):
        return ((x + k + 4) % 4) * 2 + (yl if flip == 0 else 1 - yl)

    oh = 1 - yh
    oc = 1 - core
    XP = {"grp": grp, "col": c_at(1)}
    XM = {"grp": grp, "col": c_at(-1)}
    YN = {"grp": grp, "col": c_at(0, 1)}
    ZP = {"grp": z_at(1), "col": col}
    ZM = {"grp": z_at(-1), "col": col}
    YF = {"grp": z_at(0, oh), "col": col}
    CO = {"grp": z_at(0, None, oc), "col": col}

    sends = []

    def send(src, dst, sem, to):
        cp = pltpu.make_async_remote_copy(
            src_ref=src, dst_ref=dst, send_sem=send_sem.at[len(sends)], recv_sem=sem,
            device_id=to, device_id_type=pl.DeviceIdType.MESH,
        )
        cp.start()
        sends.append(cp)

    def arrived(dst, sem):
        pltpu.make_async_remote_copy(
            src_ref=dst, dst_ref=dst, send_sem=send_sem.at[0], recv_sem=sem,
            device_id=XP, device_id_type=pl.DeviceIdType.MESH,
        ).wait_recv()

    RB = G.shape[2]
    H = RB // 2
    Q = RB // 4
    W = R.shape[1] // 2

    def g_part(s, q):
        return G.at[s, pl.ds(q * Q, Q)]

    def r_half(s, h):
        return R.at[s, pl.ds(h * W, W)]

    def send_g(s, q, to):
        send(g_part(s, q), g_part(s, q), g_sem.at[s, q], to)

    def send_r(s, h, to):
        send(r_half(s, h), r_half(s, h), r_sem.at[s, h], to)

    def got_g(s, *qs):
        for q in qs:
            arrived(g_part(s, q), g_sem.at[s, q])

    def got_r(s, *hs):
        for h in hs:
            arrived(r_half(s, h), r_sem.at[s, h])

    def send_l(g, to):
        send(L.at[g], L.at[g], l_sem.at[g], to)

    def got_l(g):
        arrived(L.at[g], l_sem.at[g])

    barrier = pltpu.get_barrier_semaphore()
    for to in (XP, XM, YN, ZP, ZM, YF, CO):
        pl.semaphore_signal(barrier, inc=1, device_id=to, device_id_type=pl.DeviceIdType.MESH)
    fetches = []
    for k, (src, dst) in enumerate((
        (grad, grad_v), (right_t, R.at[col]), (left, L.at[grp]),
        (exp_avg, avg_v), (exp_avg_sq, sq_v), (gram_left, gl_v), (gram_right, gr_v),
    )):
        cp = pltpu.make_async_copy(src, dst, in_sem.at[k])
        cp.start()
        fetches.append(cp)
    right_acc[...] = jnp.zeros_like(right_acc)
    fetches[0].wait()
    G[col] = grad_v[...].astype(B16)
    fetches[1].wait()
    fetches[2].wait()
    pl.semaphore_wait(barrier, 7)

    me = col
    xm, xp, yn = c_at(-1), c_at(1), c_at(0, 1)
    far = c_at(2)
    xm_n, xp_n, far_n = c_at(-1, 1), c_at(1, 1), c_at(2, 1)

    for h in (0, 1):
        for to in (YN, XP, XM):
            send_r(me, h, to)
    for to in (ZP, ZM, YF, CO):
        send_l(grp, to)
    send_g(me, 0, XP)
    send_g(me, 3, XM)
    send_g(me, 0, YN)

    def l_pass(g, to):
        got_l(g)
        if to is not None:
            send_l(g, to)
        send_l(g, CO)

    width = right_acc.shape[0]
    picks = lax.broadcasted_iota(jnp.int32, (width, RB), 0)
    lanes = lax.broadcasted_iota(jnp.int32, (width, RB), 1)
    chosen = jnp.where(lanes == picks + col * width, 1.0, 0.0).astype(B16)

    def right_of(s):
        rows = G[s]
        narrow = dot(chosen, rows, BY_ROWS).astype(B16)
        right_acc[...] += dot(narrow, rows)

    def pair_send(s):
        send(LP.at[pl.ds(2 * s, 2), oc], EP.at[pl.ds(2 * s, 2)], e_sem.at[s], CO)

    order = ((0, 0), (0, 1), (3, 0), (1, 0), (2, 0), (3, 1), (1, 1), (2, 1))

    def over(lo, hi, f):
        def body(i, carry):
            dx = sum(jnp.where(i == n, order[n][0], 0) for n in range(lo, hi))
            flip = sum(jnp.where(i == n, order[n][1], 0) for n in range(lo, hi))
            f(((x + dx) % 4) * 2 + (yl + flip) % 2)
            return carry

        lax.fori_loop(lo, hi, body, 0)

    def rows_of(q):
        return pl.ds(pl.multiple_of(q * Q, Q), Q)

    def half_rows(h):
        return pl.ds(h * H, H)

    def turn_h(s, h):
        T[s, half_rows(h)] = dot(G[s, half_rows(h)], R[...].reshape(RB, RB), BY_ROWS).astype(B16)

    def left_h(s, h):
        LP[2 * s + h] = dot(G[s, half_rows(h)], G[me], BY_ROWS).reshape(2, 128, RB)

    def turn_q(s, q):
        T[s, rows_of(q)] = dot(G[s, rows_of(q)], R[...].reshape(RB, RB), BY_ROWS).astype(B16)

    def left_q(s, q):
        LP[2 * s + q // 2, q % 2] = dot(G[s, rows_of(q)], G[me], BY_ROWS)

    left_h(me, 0)
    got_r(xm, 0, 1)
    send_r(xm, 0, XP)
    got_r(xp, 0, 1)
    send_r(xp, 1, XM)
    for s in (xm, xp):
        for h in (0, 1):
            send_r(s, h, YN)
    send_g(me, 1, XP)
    send_g(me, 2, XM)
    send_g(me, 1, YN)
    l_pass(z_at(-1), ZP)
    l_pass(z_at(1), ZM)
    g = z_at(0, oh)
    got_l(g)
    send_l(g, ZP)
    send_l(g, ZM)
    send_l(g, CO)
    send_g(me, 2, XP)
    send_g(me, 1, XM)
    got_g(xm, 0)
    send_g(xm, 0, XP)
    got_g(xp, 3)
    send_g(xp, 3, XM)
    left_h(me, 1)
    got_r(far, 0, 1)
    send_r(far, 0, YN)
    send_r(far, 1, YN)
    send_g(me, 2, YN)
    send_g(me, 3, YN)
    pair_send(me)
    l_pass(z_at(-2), ZP)
    l_pass(z_at(2), ZM)
    got_g(xm, 1)
    send_g(xm, 1, XP)
    got_g(xp, 2)
    send_g(xp, 2, XM)
    send_g(me, 3, XP)
    send_g(me, 0, XM)
    for q in (0, 1):
        got_g(yn, q)
        send_g(yn, q, XP)
        send_g(yn, q, XM)
    left_h(yn, 0)
    l_pass(z_at(-1, oh), ZP)
    l_pass(z_at(1, oh), ZM)
    left_h(xm, 0)
    left_h(xp, 1)
    l_pass(z_at(-3), ZP)
    l_pass(z_at(3), None)
    got_r(yn, 0, 1)
    for s in (xm_n, xp_n, far_n):
        got_r(s, 0, 1)
    turn_h(me, 0)
    turn_h(me, 1)
    got_g(yn, 2)
    send_g(yn, 2, XP)
    send_g(yn, 2, XM)
    got_g(far, 0, 3)
    send_g(far, 0, YN)
    send_g(far, 3, YN)
    l_pass(z_at(-2, oh), ZP)
    l_pass(z_at(2, oh), ZM)
    turn_h(yn, 0)
    turn_h(xm, 0)
    turn_h(xp, 1)
    got_g(yn, 3)
    send_g(yn, 3, XP)
    send_g(yn, 3, XM)
    got_g(far, 1, 2)
    send_g(far, 1, YN)
    send_g(far, 2, YN)
    l_pass(z_at(4), None)
    turn_h(yn, 1)
    left_h(yn, 1)
    pair_send(yn)
    for h in (0, 1):
        turn_h(far, h)
        left_h(far, h)
    pair_send(far)
    got_g(xm, 2, 3)
    got_g(xp, 0, 1)
    turn_h(xm, 1)
    left_h(xm, 1)
    l_pass(z_at(-3, oh), None)
    l_pass(z_at(3, oh), ZM)
    turn_h(xp, 0)
    left_h(xp, 0)
    pair_send(xm)
    pair_send(xp)

    far_order = (0, 3, 1, 2)

    def late(n, f):
        def body(i, carry):
            dx = jnp.where(i == 5, 3, jnp.where(i == 6, 1, 2))
            q = jnp.where(i == 7, far_order[n], n)
            f(((x + dx) % 4) * 2 + 1 - yl, q)
            return carry

        lax.fori_loop(5, 8, body, 0)

    def late_got(n):
        got_g(xm_n, n)
        got_g(xp_n, n)
        got_g(far_n, far_order[n])

    for n in (0, 1):
        late_got(n)
        late(n, turn_q)
        late(n, left_q)
    late_got(2)
    late(2, turn_q)
    l_pass(z_at(4, oh), None)
    late(2, left_q)
    late_got(3)
    late(3, turn_q)
    for h in (yh, oh):
        for k in range(8):
            got_l(z_at(k, h, oc))
    for h in (0, 1):
        at = pl.ds(h * H, H)
        rot[:, at] = dot(L[...].reshape(8 * RB, RB), T[:, :, at].reshape(8 * RB, H), BY_COLS)
    fetches[3].wait()
    fetches[4].wait()

    def moments(i, carry):
        at = pl.ds(i * 64, 64)
        turned = rot[at, :]
        m1 = decay * avg_v[at, :] + (1.0 - decay) * turned
        m2 = decay * sq_v[at, :] + (1.0 - decay) * turned * turned
        first[at, :] = m1
        second[at, :] = m2
        dirn[at, :] = (m1 / bias_fix / (jnp.sqrt(m2 / bias_fix) + 1e-08)).astype(B16)
        return carry

    lax.fori_loop(0, RB // 64, moments, 0)

    E = RB // 8

    def part(d, q, count=1):
        return dot(L[pl.ds(4 * d + q, count)].reshape(count * Q, RB), dirn[...])

    def at_rows(lo, n):
        return pl.ds(lo, n)

    lower, upper, rest, first_e = at_rows(0, H), at_rows(H, H), at_rows(E, H - E), at_rows(0, E)
    quarter = [at_rows(q * Q, Q) for q in range(4)]
    S1[0, lower] = part(xp_n, 0, 2).astype(B16)
    S1[1, lower] = part(xm_n, 0, 2).astype(B16)
    send(S1.at[0, rest], D1.at[0, rest], d1_sem.at[0, 0], XP)
    S1Y[lower] = part(far_n, 0, 2).astype(B16)
    send(S1.at[1, rest], D1.at[1, rest], d1_sem.at[1, 0], XM)
    S1[0, upper] = part(xp_n, 2, 2).astype(B16)
    send(S1Y.at[quarter[0]], D1Y.at[quarter[0]], d1y_sem.at[0], YN)
    S1[1, upper] = part(xm_n, 2, 2).astype(B16)
    send(S1.at[0, upper], D1.at[0, upper], d1_sem.at[0, 1], XP)
    S1Y[upper] = part(far_n, 2, 2).astype(B16)
    send(S1.at[1, upper], D1.at[1, upper], d1_sem.at[1, 1], XM)
    late(3, left_q)
    for q in (2, 1, 3):
        send(S1Y.at[quarter[q]], D1Y.at[quarter[q]], d1y_sem.at[q], YN)
    for d in (0, 1):
        send(S1.at[d, first_e], X1.at[d], x1_sem.at[d], YN)
    for s in (xm_n, xp_n, far_n):
        pair_send(s)
    fetches[5].wait()
    fetches[6].wait()

    def stat_of(half, k):
        b = half * 8 + (z + k + 8) % 8
        return LP[b, core] + EP[b]

    def stat_send(d, k, step):
        length = 4 if d == k else 3
        away = length + 1 - step
        total = stat_of(yh if k == 0 else oh, away if d == 0 else -away)
        if step > 1:
            arrived(ER.at[d, k, step - 2], er_sem.at[d, k, step - 2])
            total = total + ER[d, k, step - 2].astype(F32)
        ES[d, k, step - 1] = total.astype(B16)
        send(
            ES.at[d, k, step - 1], ER.at[d, k, step - 1], er_sem.at[d, k, step - 1],
            ZP if d == 0 else ZM,
        )

    def stat_total(k):
        total = stat_of(yh if k == 0 else oh, 0)
        for d in (0, 1):
            last = 3 if d == k else 2
            arrived(ER.at[d, k, last], er_sem.at[d, k, last])
            total = total + ER[d, k, last].astype(F32)
        return total

    S3[0, upper] = part(xp, 2, 2).astype(B16)
    S3[1, lower] = part(xm, 0, 2).astype(B16)
    for s in (me, xm, xp, yn, far, xm_n, xp_n, far_n):
        arrived(EP.at[pl.ds(2 * s, 2)], e_sem.at[s])
    for k in (1, 0):
        stat_send(0, k, 1)
        stat_send(1, k, 1)

    def second_hop(d, q):
        arrived(D1Y.at[quarter[q]], d1y_sem.at[q])
        own = quarter[q - 2 * d]
        S2[d, own] = (part(far, q) + D1Y[quarter[q]].astype(F32)).astype(B16)
        send(S2.at[d, own], D2.at[d, own], d2_sem.at[d, q - 2 * d], XP if d == 0 else XM)

    over(0, 4, right_of)
    second_hop(0, 0)
    second_hop(1, 2)
    stat_send(0, 1, 2)
    stat_send(1, 1, 2)
    second_hop(0, 1)
    second_hop(1, 3)
    send(S3.at[0, upper], D3.at[0, upper], d3_sem.at[0, 2], XP)
    send(S3.at[1, rest], D3.at[1, rest], d3_sem.at[1, 0], XM)
    stat_send(0, 0, 2)
    stat_send(1, 0, 2)
    for d in (0, 1):
        arrived(D1.at[d, upper], d1_sem.at[d, 1])
        arrived(D1.at[d, rest], d1_sem.at[d, 0])
    S2Y[upper] = (
        part(yn, 2, 2) + D1[0, upper].astype(F32) + D1[1, upper].astype(F32)
    ).astype(B16)
    own = part(yn, 0, 2)
    S2Y[first_e] = own[:E].astype(B16)
    S2Y[rest] = (own[E:] + D1[0, rest].astype(F32) + D1[1, rest].astype(F32)).astype(B16)
    send(S2Y.at[upper], D2Y.at[upper], d2y_sem.at[1], YN)
    send(S2Y.at[lower], D2Y.at[lower], d2y_sem.at[0], YN)
    over(4, 8, right_of)
    right_stat[...] = decay * gr_v[...] + (1.0 - decay) * right_acc[...]
    stat_send(0, 1, 3)
    stat_send(1, 1, 3)
    for d in (0, 1):
        arrived(X1.at[d], x1_sem.at[d])
    S3[1, first_e] = (dot(L[4 * xm, first_e], dirn[...]) + X1[1].astype(F32)).astype(B16)
    send(S3.at[1, first_e], D3.at[1, first_e], d3_sem.at[1, 1], XM)
    arrived(D2.at[0, quarter[0]], d2_sem.at[0, 0])
    own = part(xp, 0) + D2[0, quarter[0]].astype(F32)
    S3[0, first_e] = (own[:E] + X1[0].astype(F32)).astype(B16)
    S3[0, at_rows(E, Q - E)] = own[E:].astype(B16)

    def third_hop(d, q):
        mine = quarter[q - 2 * d]
        arrived(D2.at[d, mine], d2_sem.at[d, q - 2 * d])
        S3[d, quarter[q]] = (
            part(xp if d == 0 else xm, q) + D2[d, mine].astype(F32)
        ).astype(B16)

    def third_send(d, q):
        send(
            S3.at[d, quarter[q]], D3.at[d, quarter[q]], d3_sem.at[d, q],
            XP if d == 0 else XM,
        )

    third_hop(1, 2)
    third_send(0, 0)
    third_send(1, 2)
    stat_send(0, 0, 3)
    third_hop(0, 1)
    third_send(0, 1)
    third_hop(1, 3)
    third_send(1, 3)
    stat_send(1, 1, 4)
    stat_send(1, 0, 3)
    stat_send(0, 0, 4)
    AO[...] = stat_total(1).astype(B16)
    send(AO, YB, yb_sem.at[0], YF)
    rot[...] = part(me, 0, 4)
    left_stat[...] = decay * gl_v[...] + (1.0 - decay) * stat_total(0)
    arrived(D2Y.at[upper], d2y_sem.at[1])
    arrived(D2Y.at[lower], d2y_sem.at[0])
    arrived(D3.at[0, upper], d3_sem.at[0, 2])
    arrived(D3.at[1, rest], d3_sem.at[1, 0])
    arrived(D3.at[1, first_e], d3_sem.at[1, 1])
    rot[upper] += D2Y[upper].astype(F32) + D3[0, upper].astype(F32)
    rot[lower] += D2Y[lower].astype(F32) + D3[1, lower].astype(F32)
    for q in (0, 1):
        arrived(D3.at[0, quarter[q]], d3_sem.at[0, q])
        arrived(D3.at[1, quarter[q + 2]], d3_sem.at[1, q + 2])
    basis = R[...].reshape(RB, RB)
    update[lower] = dot((rot[lower] + D3[0, lower].astype(F32)).astype(B16), basis)
    update[upper] = dot((rot[upper] + D3[1, upper].astype(F32)).astype(B16), basis)
    arrived(YB, yb_sem.at[0])
    left_stat[...] += (1.0 - decay) * YB[...].astype(F32)
    for cp in sends:
        cp.wait_send()


def put_out(*refs):
    held, out, sem = refs[:5], refs[5:10], refs[10]
    copies = [pltpu.make_async_copy(a, b, sem.at[k]) for k, (a, b) in enumerate(zip(held, out))]
    for cp in copies:
        cp.start()
    for cp in copies:
        cp.wait()


def local(grad, exp_avg, exp_avg_sq, left_basis, right_basis, gram_left, gram_right):
    rows, RB = grad.shape
    assert rows == RB
    H = RB // 2
    width = right_basis.shape[1]
    vm = pltpu.VMEM
    dma = pltpu.SemaphoreType.DMA
    scratch = [
        vm((RB, RB), F32), vm((RB, RB), F32), vm((RB, RB), F32), vm((128, RB), F32), vm((width, RB), F32),
        vm((8, RB, RB), B16),
        vm((8, width, RB), B16),
        vm((32, 128, RB), B16),
        vm((8, RB, RB), B16),
        vm((16, 2, 128, RB), F32),
        vm((16, 128, RB), F32),
        vm((RB, RB), F32),
        vm((width, RB), F32),
        vm((RB, RB), B16),
        vm((2, 2, 4, 128, RB), B16),
        vm((2, 2, 4, 128, RB), B16),
        vm((128, RB), B16),
        vm((128, RB), B16),
        vm((2, RB, RB), B16),
        vm((RB, RB), B16),
        vm((2, RB // 8, RB), B16),
        vm((2, H, RB), B16),
        vm((RB, RB), B16),
        vm((2, RB, RB), B16),
        vm((2, RB, RB), B16),
        vm((RB, RB), B16),
        vm((2, H, RB), B16),
        vm((RB, RB), B16),
        vm((2, RB, RB), B16),
        dma((7,)), dma((160,)), dma((8, 4)), dma((8, 2)), dma((32,)), dma((8,)), dma((2, 2, 4)),
        dma((1,)), dma((2, 2)), dma((4,)), dma((2,)), dma((2, 2)), dma((2,)), dma((2, 4)),
    ]
    whole = pl.BlockSpec(memory_space=pl.ANY)
    like = lambda a: pltpu.VMEM(a.shape, F32)
    gram_rt = gram_right.T
    update, first, second, left_stat, right_rt = pl.pallas_call(
        kernel,
        out_shape=(like(grad), like(grad), like(grad), like(gram_left), like(gram_rt)),
        in_specs=[whole] * 7,
        out_specs=(pl.BlockSpec(memory_space=pltpu.VMEM),) * 5,
        scratch_shapes=scratch,
        compiler_params=pltpu.CompilerParams(
            collective_id=0, has_side_effects=True, vmem_limit_bytes=58 * 1024 * 1024
        ),
    )(grad, exp_avg, exp_avg_sq, left_basis, right_basis.T, gram_left, gram_rt)
    results = (update, first, second, left_stat, right_rt)
    update, first, second, left_stat, right_rt = pl.pallas_call(
        put_out,
        out_shape=tuple(jax.ShapeDtypeStruct(a.shape, F32) for a in results),
        in_specs=[pl.BlockSpec(memory_space=pltpu.VMEM)] * 5,
        out_specs=(whole,) * 5,
        scratch_shapes=[dma((5,))],
        compiler_params=pltpu.CompilerParams(vmem_limit_bytes=2 * 1024 * 1024),
    )(*results)
    return update, first, second, left_stat, right_rt.T


def solution(mesh):
    a, b = P("col", "grp"), P("grp", "col")
    return jax.shard_map(
        local, mesh=mesh, in_specs=(a, a, a, b, b, b, b), out_specs=(a, a, a, b, b), check_vma=False
    )
```
